32 devices in a mesh: gz: 8 (over y, x, core), gx: 4 (over z).
Axes of the slice: x: 2, y: 2, z: 4, core: 2. Of those that a mesh axis runs over, the one named last changes fastest.
Arguments:
- density: float32 [512, 128, 128], P('gz', 'gx'), may hold values from -6 to 6
- velocity: float32 [3, 512, 128, 128], P(None, 'gz', 'gx'), may hold values from -6 to 6
- labels: int32 [512, 128, 128], P('gz', 'gx'), may hold values from 0 to 7
- sound_table: float32 [8], replicated, may hold values from 0.8 to 1.6
- mass_table: float32 [8], replicated, may hold values from 0.8 to 2
- source_index: int32 [4096], replicated, may hold values from 0 to 8388607
- source_values: float32 [1, 4096], replicated, may hold values from -6 to 6
Outputs:
- new_density: float32 [512, 128, 128], P('gz', 'gx')
- new_velocity: float32 [3, 512, 128, 128], P(None, 'gz', 'gx')
The draws below stay inside these ranges and needn't reach their ends.
Inputs may be any that keep to these rules, and one draw needn't show every extreme that they name: `source_index`: flat cell index z * 128 * 128 + x * 128 + y; an index may repeat.
All inputs are finite; a program needn't handle non-finite values.
Results may differ from the reference program's by a relative error of at most 0.00011.
Values sent between devices are 32-bit elements; how exact they have to be, the bound alone decides.
A program may use at most 128 MiB of HBM per device.

```python
import math
import jax
import jax.numpy as jnp

NZ = 512
NX = 128
NY = 128
LABELS = 8
PML_W = 20
STEPS = 1
SRC = 4096


def with_ends(drawn, key, smallest, top_value):
    longest = drawn.shape.index(max(drawn.shape))
    spots = []
    for shift in (0, 1):
        where = [jax.random.randint(jax.random.fold_in(key, axis), (), 0, length) for axis, length in enumerate(drawn.shape)]
        where[longest] = (where[longest] + shift) % drawn.shape[longest]
        spots.append(tuple(where))
    return drawn.at[spots[0]].set(smallest).at[spots[1]].set(top_value)


def level_of(stream_key, extent, shards, low, top_value):
    def one(position, shards_of):
        heights = jax.random.uniform(jax.random.fold_in(jax.random.fold_in(stream_key, 6), position), (shards_of,), jnp.float32, low / len(shards), top_value / len(shards))
        return jnp.repeat(jnp.exp(heights), extent[position] // shards_of).reshape((-1,) + (1,) * (len(extent) - position - 1))

    factor_of = one(*shards[0])
    for cut in shards[1:]:
        factor_of = factor_of * one(*cut)
    return factor_of


def gaussian(stream_key, dims, width, reach, shards=(), kind=jnp.bfloat16):
    drawn = jax.random.normal(stream_key, dims, jnp.float32) * width
    if len(shards) > 0:
        drawn = level_of(stream_key, dims, shards, -0.22, 0.18) * drawn
    return jnp.clip(drawn, min=-reach, max=reach).astype(kind)


def setup_inputs(seed: int = 0) -> dict:
    seeds = jax.random.split(jax.random.key(seed), 8)
    density = gaussian(seeds[0], (NZ, NX, NY), 1.0, 6.0, ((0, 8), (1, 4)), jnp.float32)
    velocity = gaussian(seeds[1], (3, NZ, NX, NY), 1.0, 6.0, ((1, 8), (2, 4)), jnp.float32)
    labels = with_ends(jax.random.randint(seeds[2], (NZ, NX, NY), 0, LABELS), jax.random.fold_in(seeds[2], 1), 0, LABELS - 1).astype(jnp.int32)
    sound_table = jnp.clip(jax.random.uniform(seeds[3], (LABELS,), jnp.float32, 0.8, 1.6), 0.8, 1.6)
    mass_table = jnp.clip(jax.random.uniform(seeds[4], (LABELS,), jnp.float32, 0.8, 2.0), 0.8, 2.0)
    source_index = with_ends(jax.random.randint(seeds[5], (SRC,), 0, NX * NY * NZ), jax.random.fold_in(seeds[5], 1), 0, (NX * NY * NZ) - 1).astype(jnp.int32)
    source_values = gaussian(seeds[6], (STEPS, SRC), 1.0, 6.0, (), jnp.float32)
    return {"density": density, "velocity": velocity, "labels": labels, "sound_table": sound_table, "mass_table": mass_table, "source_index": source_index, "source_values": source_values}


time_step = 0.3
absorb = 2.0

def wavenumber(length):
    positions = jnp.arange(length, dtype=jnp.int32)
    signed = jnp.where(positions < length // 2, positions, positions - length)
    return 2.0 * math.pi / length * signed.astype(jnp.float32)

def damping(length, speed_ref):
    coordinate = jnp.arange(length, dtype=jnp.int32).astype(jnp.float32)
    layer_depth = jnp.maximum(jnp.maximum(PML_W - coordinate, coordinate - (length - 1 - PML_W)), 0.0) / PML_W
    return jnp.exp(-absorb * speed_ref * layer_depth ** 4 * time_step * 0.5)

def reference(density, velocity, labels, sound_table, mass_table, source_index, source_values):
    speed_sq = sound_table[labels] ** 2
    rho_zero = mass_table[labels]
    speed_ref = jnp.max(sound_table)
    wave_list = (wavenumber(NZ)[:, None, None], wavenumber(NX)[None, :, None], wavenumber(NY)[None, None, :])
    magnitude = jnp.sqrt(wave_list[0] ** 2 + wave_list[1] ** 2 + wave_list[2] ** 2)
    correction = jnp.sinc(speed_ref * magnitude * time_step / (2.0 * math.pi))
    damp_list = (damping(NZ, speed_ref)[:, None, None], damping(NX, speed_ref)[None, :, None], damping(NY, speed_ref)[None, None, :])
    damp_all = damp_list[0] * damp_list[1] * damp_list[2]
    for moment in range(STEPS):
        pressure = speed_sq * density
        spectrum = jnp.fft.fftn(pressure) * correction
        updated = []
        for direction in range(3):
            factor = 1j * wave_list[direction] * jnp.exp(0.5j * wave_list[direction])
            gradient_part = jnp.real(jnp.fft.ifftn(spectrum * factor))
            updated.append(damp_list[direction] * (damp_list[direction] * velocity[direction] - time_step / rho_zero * gradient_part))
        velocity = jnp.stack(updated)
        summed = None
        for direction in range(3):
            factor = 1j * wave_list[direction] * jnp.exp(-0.5j * wave_list[direction])
            contribution = jnp.fft.fftn(velocity[direction]) * factor
            summed = contribution if summed is None else summed + contribution
        spread = jnp.real(jnp.fft.ifftn(summed * correction))
        density = damp_all * (damp_all * density - time_step * rho_zero * spread)
        density = density.reshape(-1).at[source_index].add(source_values[moment]).reshape(density.shape)
    return (density, velocity)
```

```python
import functools
import math

import numpy as np

import jax
import jax.numpy as jnp
from jax import lax
from jax.experimental import pallas as pl
from jax.experimental.pallas import tpu as pltpu
from jax.sharding import PartitionSpec as P

NZ = 512
NX = 128
NY = 128
LABELS = 8
PML_W = 20


time_step = 0.3
absorb = 2.0
high = lax.Precision.HIGHEST


def damping(positions, length, speed_ref):
    coordinate = positions.astype(jnp.float32)
    layer_depth = (
        jnp.maximum(jnp.maximum(PML_W - coordinate, coordinate - (length - 1 - PML_W)), 0.0) / PML_W
    )
    return jnp.exp(-absorb * speed_ref * layer_depth**4 * time_step * 0.5)


def add_sources(density, source_index, amounts, z_start, x_start):
    z_local, x_local, y_count = density.shape
    plane_size = NX * NY
    z_offset = source_index // plane_size - z_start
    remain = source_index % plane_size
    x_offset = remain // NY - x_start
    y_offset = remain % NY
    inside = (z_offset >= 0) & (z_offset < z_local) & (x_offset >= 0) & (x_offset < x_local)
    flat_index = jnp.where(
        inside, (z_offset * x_local + x_offset) * y_count + y_offset, z_local * x_local * y_count
    )
    return density.reshape(-1).at[flat_index].add(amounts, mode="drop").reshape(density.shape)


def real_basis(length):
    cells = np.arange(length)
    columns = np.zeros((length, length))
    waves = np.zeros(length)
    half = length // 2
    for index in range(half):
        angle = 2 * np.pi * index / length
        if index == 0:
            columns[:, 0] = 1 / np.sqrt(length)
            columns[:, 1] = np.cos(np.pi * cells) / np.sqrt(length)
            waves[1] = np.pi
        else:
            columns[:, 2 * index] = np.cos(angle * cells) * np.sqrt(2 / length)
            columns[:, 2 * index + 1] = np.sin(angle * cells) * np.sqrt(2 / length)
            waves[2 * index : 2 * index + 2] = angle
    return columns, waves


def staggered(length, orient):
    index = np.arange(length)
    wave = 2 * np.pi / length * np.where(index < length // 2, index, index - length)
    kernel = np.fft.ifft(1j * wave * np.exp(0.5j * orient * wave)).real
    return kernel[(index[:, None] - index[None, :]) % length]


def line_tables(length):
    basis, waves = real_basis(length)
    plus = staggered(length, 1.0) @ basis
    minus = staggered(length, -1.0).T @ basis
    return tuple(np.asarray(t, np.float32) for t in (basis, plus, minus)) + (waves,)


def contract(formula, operand, matrix):
    return jnp.einsum(formula, operand, matrix, precision=high, preferred_element_type=jnp.float32)


def packed_table(table, pack, z_devices):
    z_local = table.shape[0] // z_devices
    blocks = table.reshape(z_devices, 1, z_local, 1, table.shape[1])
    lines = np.eye(pack, dtype=np.float32).reshape(1, pack, 1, pack, 1)
    return (blocks * lines).reshape(z_devices, pack * z_local, pack * table.shape[1])


def exchange_kernel(axis, size, count, *refs):
    sources, targets = refs[:count], refs[count : 2 * count]
    held = refs[2 * count : 3 * count]
    send_sem, recv_sem, in_sem, out_sem = refs[3 * count :]
    me = lax.axis_index(axis)
    barrier = pltpu.get_barrier_semaphore()
    for step in range(1, size):
        pl.semaphore_signal(
            barrier,
            inc=1,
            device_id={axis: lax.rem(me + step, size)},
            device_id_type=pl.DeviceIdType.MESH,
        )
    locals_in = [
        pltpu.make_async_copy(sources[f].at[me], held[f], in_sem.at[f]) for f in range(count)
    ]
    for copy in locals_in:
        copy.start()
    pl.semaphore_wait(barrier, size - 1)
    copies = []
    for f in range(count):
        for step in range(1, size):
            peer = lax.rem(me + step, size)
            copy = pltpu.make_async_remote_copy(
                src_ref=sources[f].at[peer],
                dst_ref=targets[f].at[me],
                send_sem=send_sem.at[f, step],
                recv_sem=recv_sem.at[f, step],
                device_id={axis: peer},
                device_id_type=pl.DeviceIdType.MESH,
            )
            copy.start()
            copies.append(copy)
    locals_out = []
    for f in range(count):
        locals_in[f].wait()
        copy = pltpu.make_async_copy(held[f], targets[f].at[me], out_sem.at[f])
        copy.start()
        locals_out.append(copy)
    for copy in locals_out + copies:
        copy.wait()


def exchange(axis, size, name, *fields):
    count = len(fields)
    anywhere = pl.BlockSpec(memory_space=pl.ANY)
    return pl.pallas_call(
        functools.partial(exchange_kernel, axis, size, count),
        out_shape=[jax.ShapeDtypeStruct(f.shape, f.dtype) for f in fields],
        in_specs=[anywhere] * count,
        out_specs=[anywhere] * count,
        scratch_shapes=[pltpu.VMEM(f.shape[1:], f.dtype) for f in fields]
        + [
            pltpu.SemaphoreType.DMA((count, size)),
            pltpu.SemaphoreType.DMA((count, size)),
            pltpu.SemaphoreType.DMA((count,)),
            pltpu.SemaphoreType.DMA((count,)),
        ],
        compiler_params=pltpu.CompilerParams(collective_id=name, has_side_effects=True),
        name=f"exchange_{axis}_{name}",
    )(*fields)


def shards(density, velocity, labels, sound_table, mass_table, source_index, source_values):
    z_local, x_local, y_count = density.shape
    z_devices, x_devices = lax.axis_size("gz"), lax.axis_size("gx")
    z_start = lax.axis_index("gz") * z_local
    x_start = lax.axis_index("gx") * x_local
    speed_sq = jnp.zeros(density.shape, jnp.float32)
    rho_zero = jnp.zeros(density.shape, jnp.float32)
    for tissue in range(LABELS):
        chosen = labels == tissue
        speed_sq = jnp.where(chosen, sound_table[tissue] ** 2, speed_sq)
        rho_zero = jnp.where(chosen, mass_table[tissue], rho_zero)
    speed_ref = jnp.max(sound_table)
    damp_z = damping(z_start + jnp.arange(z_local, dtype=jnp.int32), NZ, speed_ref)[:, None, None]
    damp_x = damping(x_start + jnp.arange(x_local, dtype=jnp.int32), NX, speed_ref)[None, :, None]
    damp_y = damping(jnp.arange(y_count, dtype=jnp.int32), NY, speed_ref)[None, None, :]
    damp_all = damp_z * damp_x * damp_y
    z_basis, z_plus, z_minus, z_waves = line_tables(NZ)
    x_basis, x_plus, x_minus, x_waves = line_tables(NX)
    y_basis, y_plus, y_minus, y_waves = line_tables(NY)
    kx_local, ky_local = NX // z_devices, NY // x_devices
    pack = 2 if 2 * z_local <= 128 else 1
    groups = ky_local // pack
    lanes = pack * z_local
    z_tables = [packed_table(t, pack, z_devices) for t in (z_basis, z_plus, z_minus)]
    x_tables = [t.reshape(x_devices, x_local, z_devices, kx_local) for t in (x_basis, x_plus, x_minus)]
    y_tables = [t.reshape(y_count, x_devices * groups, pack) for t in (y_basis, y_plus, y_minus)]
    wave_x = lax.dynamic_slice_in_dim(
        jnp.asarray(x_waves, jnp.float32), lax.axis_index("gz") * kx_local, kx_local
    )[None, :, None]
    wave_y = lax.dynamic_slice_in_dim(
        jnp.asarray(y_waves, jnp.float32), lax.axis_index("gx") * ky_local, ky_local
    ).reshape(groups, 1, pack)
    wave_y = jnp.repeat(wave_y, NZ, axis=2)
    wave_z = jnp.asarray(np.tile(z_waves, pack), jnp.float32)[None, None, :]
    correction = jnp.sinc(
        speed_ref * jnp.sqrt(wave_z**2 + wave_x**2 + wave_y**2) * time_step / (2.0 * math.pi)
    )

    def y_forward(field, table):
        out = contract("zxy,yqp->qxpz", field, y_tables[table])
        return out.reshape(x_devices, groups, x_local, lanes)

    def x_forward(blocks, table):
        return contract("iqxl,ixdm->dqml", blocks, x_tables[table])

    def z_forward(blocks, table):
        return contract("dqml,dlc->qmc", blocks, z_tables[table])

    def z_inverse(spectrum, table):
        return contract("qmc,dlc->dqml", spectrum, z_tables[table])

    def x_inverse(blocks, table):
        return contract("dqml,ixdm->iqxl", blocks, x_tables[table])

    def y_inverse(blocks, table):
        blocks = blocks.reshape(x_devices * groups, x_local, pack, z_local)
        return contract("qxpz,yqp->zxy", blocks, y_tables[table])

    pressure = speed_sq * density
    (part,) = exchange("gx", x_devices, 0, y_forward(pressure, 0))
    (part,) = exchange("gz", z_devices, 1, x_forward(part, 0))
    spectrum = z_forward(part, 0) * correction
    along, plain = exchange("gz", z_devices, 2, z_inverse(spectrum, 1), z_inverse(spectrum, 0))
    along, across, plain = exchange(
        "gx", x_devices, 3, x_inverse(along, 0), x_inverse(plain, 1), x_inverse(plain, 0)
    )
    slope_z = y_inverse(along, 0)
    slope_x = y_inverse(across, 0)
    slope_y = y_inverse(plain, 1)
    ratio = time_step / rho_zero
    new_z = damp_z * (damp_z * velocity[0] - ratio * slope_z)
    new_x = damp_x * (damp_x * velocity[1] - ratio * slope_x)
    new_y = damp_y * (damp_y * velocity[2] - ratio * slope_y)
    along, across, plain = exchange(
        "gx", x_devices, 4, y_forward(new_z, 0), y_forward(new_x, 0), y_forward(new_y, 2)
    )
    along, plain = exchange(
        "gz", z_devices, 5, x_forward(along, 0), x_forward(across, 2) + x_forward(plain, 0)
    )
    spectrum = (z_forward(along, 2) + z_forward(plain, 0)) * correction
    (part,) = exchange("gz", z_devices, 6, z_inverse(spectrum, 0))
    (part,) = exchange("gx", x_devices, 7, x_inverse(part, 0))
    spread = y_inverse(part, 0)
    density = damp_all * (damp_all * density - time_step * rho_zero * spread)
    density = add_sources(density, source_index, source_values[0], z_start, x_start)
    return (density, jnp.stack([new_z, new_x, new_y]))


def solution(mesh):
    in_specs = (
        P("gz", "gx", None),
        P(None, "gz", "gx", None),
        P("gz", "gx", None),
        P(),
        P(),
        P(),
        P(),
    )
    out_specs = (P("gz", "gx", None), P(None, "gz", "gx", None))
    return jax.shard_map(shards, mesh=mesh, in_specs=in_specs, out_specs=out_specs, check_vma=False)
```
